32 devices in a mesh: src: 4 (over x, core), tgt: 8 (over z, y).
Axes of the slice: x: 2, y: 2, z: 4, core: 2. Of those that a mesh axis runs over, the one named last changes fastest.
Arguments:
- coefficients: bfloat16 [4, 8, 512, 512], P('src', 'tgt'), may hold values from -6 to 6
- transfer_blocks: bfloat16 [4, 4, 8, 512, 1024], P(None, 'src', 'tgt'), may hold values from -0.1875 to 0.1875
Outputs:
- result: bfloat16 [4, 8, 512, 512], P('src', 'tgt')
The draws below stay inside these ranges and needn't reach their ends.
All inputs are finite; a program needn't handle non-finite values.
Results may differ from the reference program's by a relative error of at most 0.0064.
Values may be sent and summed in bfloat16 or wider, within the bound.
No kernel may reach another device: no remote copies, remote signals or barrier semaphores. Data moves between devices by JAX's collectives and lax.ppermute only.
A program may use at most 64 MiB of HBM per device.

```python
import jax
import jax.numpy as jnp
from jax import lax

RANK = 512
COLS = 512
LEVELS = 4
N_SRC = 4
N_TGT = 8


def steps_of(rng, shape, shards, smallest, top_value):
    gain = 1.0
    for dim, shards_of in shards:
        steps = jax.random.uniform(jax.random.fold_in(jax.random.fold_in(rng, 6), dim), (shards_of,), jnp.float32, smallest / len(shards), top_value / len(shards))
        gain = gain * jnp.repeat(jnp.exp(steps), shape[dim] // shards_of).reshape((-1,) + (1,) * (len(shape) - 1 - dim))
    return gain


def scatter_about(stream_key, shape, scale, most, shards=(), kind=jnp.bfloat16):
    entries = jax.random.normal(stream_key, shape, jnp.float32) * scale
    if len(shards) > 0:
        entries = steps_of(stream_key, shape, shards, -0.22, 0.18) * entries
    return jnp.clip(entries, min=-most, max=most).astype(kind)


def setup_inputs(seed: int = 0) -> dict:
    streams_of = jax.random.split(jax.random.key(seed), 3)
    return {
        "coefficients": scatter_about(streams_of[0], (N_SRC, N_TGT, RANK, COLS), 1.0, 6.0, ((0, 4), (1, 8))),
        "transfer_blocks": scatter_about(streams_of[1], (LEVELS, N_SRC, N_TGT, RANK, 2 * RANK), (2 * RANK) ** -0.5, 0.1875, ((1, 4), (2, 8))),
    }


def level(current, blocks, axis, bit):
    length = current.shape[axis]
    indices = jnp.arange(length, dtype=jnp.int32)
    low_index = (indices & (~(1 << bit))).astype(jnp.int32)
    high_index = (indices | (1 << bit)).astype(jnp.int32)
    low_half = jnp.take(current, low_index, axis=axis)
    high_half = jnp.take(current, high_index, axis=axis)
    stacked = jnp.concatenate([low_half, high_half], axis=2)

    def apply_group(operand_pair):
        block_now, stack_now = operand_pair
        product = jnp.einsum("tij,tjc->tic", block_now.astype(jnp.float32), stack_now.astype(jnp.float32))
        return product.astype(jnp.bfloat16)

    return lax.map(apply_group, (blocks, stacked))


def reference(coefficients, transfer_blocks):
    src_top = N_SRC.bit_length() - 2
    tgt_top = N_TGT.bit_length() - 2
    slab_rows = RANK // N_TGT
    current = level(coefficients, transfer_blocks[0], 0, 0)
    current = level(current, transfer_blocks[1], 0, src_top)
    current = current.reshape(N_SRC, N_TGT, N_TGT, slab_rows, COLS)
    current = current.transpose(0, 2, 1, 3, 4).reshape(N_SRC, N_TGT, RANK, COLS)
    current = level(current, transfer_blocks[2], 1, tgt_top)
    current = level(current, transfer_blocks[3], 1, 0)
    return current
```

```python
import jax
import jax.numpy as jnp
from jax import lax
from jax.experimental import pallas as pl
from jax.experimental.pallas import tpu as pltpu
from jax.sharding import PartitionSpec as P

WIDTHS = (1, 1)
PLANS = ("R", "R")
LANES = 128
VM = pl.BlockSpec(memory_space=pltpu.VMEM)
SM = pl.BlockSpec(memory_space=pltpu.SMEM)


def call(kernel, shapes, operands, flops, scratch=(), specs=None):
    size = sum(o.size * o.dtype.itemsize for o in operands)
    return pl.pallas_call(
        kernel,
        out_shape=shapes,
        in_specs=[SM] + [VM] * (len(operands) - 1),
        out_specs=[VM] * len(shapes),
        scratch_shapes=list(scratch),
        compiler_params=pltpu.CompilerParams(vmem_limit_bytes=6 << 20),
        cost_estimate=pl.CostEstimate(flops=flops, bytes_accessed=size, transcendentals=0),
    )(*operands)


def pair_product(upper, block_ref, own, partner):
    half = own.shape[0]
    here = pl.multiple_of(upper * half, half)
    there = pl.multiple_of((1 - upper) * half, half)
    total = jnp.dot(block_ref[:, pl.ds(here, half)], own, preferred_element_type=jnp.float32)
    return total + jnp.dot(block_ref[:, pl.ds(there, half)], partner, preferred_element_type=jnp.float32)


def window(ref, first, width):
    return ref[...] if ref.shape[1] == width else ref[:, pl.ds(first, width)]


def pair_level(upper, block, own, partner, first, width):
    def kernel(upper_ref, block_ref, own_ref, partner_ref, out_ref):
        total = pair_product(upper_ref[0], block_ref, window(own_ref, first, width), window(partner_ref, first, width))
        out_ref[...] = total.astype(out_ref.dtype)

    shape = jax.ShapeDtypeStruct((block.shape[0], width), own.dtype)
    return call(kernel, [shape], (upper, block, own, partner), 2 * block.size * width)[0]


def pair_level_slabs(scalars, block, own, partner, count, groups):
    width = own.shape[1]
    slab = block.shape[0] // count

    def kernel(scalars_ref, block_ref, own_ref, partner_ref, *refs):
        held = refs[-1]
        held[...] = pair_product(scalars_ref[0], block_ref, own_ref[...], partner_ref[...]).astype(held.dtype)
        for out_ref, labels in zip(refs, groups):
            for place, (_, target) in enumerate(labels):
                row = pl.multiple_of((scalars_ref[1] ^ target) * slab, slab)
                out_ref[place] = held[pl.ds(row, slab), :]

    shapes = [jax.ShapeDtypeStruct((len(g), slab, width), own.dtype) for g in groups]
    outs = call(kernel, shapes, (scalars, block, own, partner), 2 * block.size * width, [pltpu.VMEM((block.shape[0], width), own.dtype)])
    return list(zip(outs, groups))


def gather(scalars, held, groups):
    arrays = [a for a, _ in held]
    at = {label: (i, k) for i, (_, labels) in enumerate(held) for k, label in enumerate(labels)}

    def kernel(scalars_ref, *refs):
        for out_ref, labels in zip(refs[len(arrays):], groups):
            for place, label in enumerate(labels):
                i, k = at[label]
                out_ref[place] = refs[i][k]

    shapes = [jax.ShapeDtypeStruct((len(g),) + arrays[0].shape[1:], arrays[0].dtype) for g in groups]
    outs = call(kernel, shapes, (scalars, *arrays), 1 << 26)
    return list(zip(outs, groups))


def stack_level(scalars, block, held, count):
    arrays = [a for a, _ in held]
    _, slab, width = arrays[0].shape
    top = count >> 1

    def kernel(scalars_ref, block_ref, *refs):
        out_ref, stack = refs[-2:]
        for ref, (_, labels) in zip(refs, held):
            for place, (source, target) in enumerate(labels):
                if target & ~top:
                    continue
                place_now = scalars_ref[1] ^ target
                upper = (place_now >= top).astype(jnp.int32)
                row = pl.multiple_of((upper * count + (scalars_ref[1] ^ source)) * slab, slab)
                stack[pl.ds(row, slab), :] = ref[place]
        out_ref[...] = jnp.dot(block_ref[...], stack[...], preferred_element_type=jnp.float32).astype(out_ref.dtype)

    shape = jax.ShapeDtypeStruct((block.shape[0], width), arrays[0].dtype)
    return call(kernel, [shape], (scalars, block, *arrays), 2 * block.size * width, [pltpu.VMEM((block.shape[1], width), arrays[0].dtype)])[0]


def flip(value, axis, mask):
    return lax.ppermute(value, axis, [(i, i ^ mask) for i in range(lax.axis_size(axis))])


def flip_slabs(held, mask):
    array, labels = held
    return flip(array, "tgt", mask), [(a ^ mask, p ^ mask) for a, p in labels]


def regroup(plan, scalars, block, own, partner, count):
    top = count >> 1
    every = list(range(count))
    if plan == "R":
        bits = [1 << b for b in range(top.bit_length() - 1)]
        first = bits[0] if bits else 0
        groups = [[(0, p) for p in every if p & first], [(0, p) for p in every if not p & first]] if bits else [[(0, p) for p in every]]
        made = pair_level_slabs(scalars, block, own, partner, count, groups)
        held = made[1:] if bits else made
        sent = made[0]
        for n, bit in enumerate(bits):
            held = held + [flip_slabs(sent, bit)]
            after = bits[n + 1] if n + 1 < len(bits) else 0
            labels = [l for _, ls in held for l in ls]
            if after:
                sent, kept = gather(scalars, held, [[l for l in labels if l[1] & after], [l for l in labels if not l[1] & after]])
                held = [kept]
            else:
                held = gather(scalars, held, [labels])
        return held + [flip_slabs(held[0], top)]
    if plan == "F":
        made = pair_level_slabs(scalars, block, own, partner, count, [[(0, p) for p in every]])
        held = made + [flip_slabs(made[0], top)]
        for b in range(top.bit_length() - 1):
            bit = 1 << b
            labels = [l for _, ls in held for l in ls]
            sent, kept = gather(scalars, held, [[l for l in labels if l[1] & bit], [l for l in labels if not l[1] & bit]])
            held = [kept, flip_slabs(sent, bit)]
        return held
    if plan == "P":
        made = pair_level_slabs(scalars, block, own, partner, count, [[(0, p) for p in every if p & 1], [(0, p) for p in every if not p & 1]])
        held = [made[1], flip_slabs(made[0], 1)]
        labels = [l for _, ls in held for l in ls]
        lows = [m for m in range(0, top, 2)]
        parts = gather(scalars, held, [[l for l in labels if l[1] & ~top == low] for low in lows])
        moved = []
        for low, part in zip(lows, parts):
            moved.append(flip_slabs(part, low | top))
            if low:
                moved.append(flip_slabs(part, low))
        return [parts[0]] + moved


def shards(coefficients, transfer_blocks):
    current = coefficients[0, 0]
    rows, columns = current.shape
    count = lax.axis_size("tgt")
    top = lax.axis_size("src").bit_length() - 2
    s, t = lax.axis_index("src"), lax.axis_index("tgt")
    s0 = (s & 1).reshape(1)
    s1 = jnp.stack([s >> top & 1, t])
    s3 = (t & 1).reshape(1)
    blocks = [transfer_blocks[0, 0, 0]]
    partner = flip(current, "src", 1)
    unit = columns // sum(WIDTHS)
    first = 0
    chunks = []
    for w in WIDTHS:
        chunks.append(pair_level(s0, blocks[0], current, partner, first, w * unit))
        first += w * unit
    later, chunks[0] = lax.optimization_barrier((transfer_blocks, chunks[0]))
    blocks += [later[k, 0, 0] for k in range(1, 4)]
    outs = []
    for plan, c in zip(PLANS, chunks):
        p = flip(c, "src", 1 << top)
        held = regroup(plan, s1, blocks[1], c, p, count)
        c = stack_level(s1, blocks[2], held, count)
        p = flip(c, "tgt", 1)
        outs.append(pair_level(s3, blocks[3], c, p, 0, c.shape[1]))
    return jnp.concatenate(outs, 1)[None, None]


def solution(mesh):
    return jax.shard_map(
        shards,
        mesh=mesh,
        in_specs=(P("src", "tgt", None, None), P(None, "src", "tgt", None, None)),
        out_specs=P("src", "tgt", None, None),
        check_vma=False,
    )
```
